32 devices in a mesh: section: 4 (over y, x), expert: 8 (over z, core).
Axes of the slice: x: 2, y: 2, z: 4, core: 2. Of those that a mesh axis runs over, the one named last changes fastest.
Arguments:
- tokens: bfloat16 [8, 64, 2048], P(None, 'expert'), may hold values from -6 to 6
- norm_gain: float32 [2, 2048], replicated, may hold values from 0.1 to 1.9
- w_gate: bfloat16 [4, 2048, 14336], P('section', None, 'expert'), may hold values from -0.125 to 0.125
- w_up: bfloat16 [4, 2048, 14336], P('section', None, 'expert'), may hold values from -0.125 to 0.125
- w_down: bfloat16 [4, 14336, 2048], P('section', 'expert'), may hold values from -0.0625 to 0.0625
- expert_ids: int32 [2, 8, 64, 2], P(None, None, 'expert'), may hold values from 0 to 3, as said below
- slot_ids: int32 [2, 8, 64, 2], P(None, None, 'expert'), may hold values from 0 to 4, as said below
- dropped: int32 [2, 8, 64, 2], P(None, None, 'expert'), may hold values from 0 to 1, as said below
- gate_weights: float32 [2, 8, 64, 2], P(None, None, 'expert'), may hold values from 0.1 to 1
Outputs:
- states: bfloat16 [4, 8, 64, 2048], P('section', None, 'expert')
The draws below stay inside these ranges and needn't reach their ends.
Inputs may be any that keep to these rules, and one draw needn't show every extreme that they name: `expert_ids`: the two experts of a token differ. `slot_ids`: among the kept choices of the tokens of one index of expert that name one expert, the slots are 0, 1, ... up to their count less one, each once. At most 5 kept choices of the tokens of one index of expert name one expert, and a choice is dropped only where 5 kept choices of its index of expert name its expert; in each layer and micro-batch some expert receives exactly 5 kept choices from every index of expert.
All inputs are finite; a program needn't handle non-finite values.
Results may differ from the reference program's by a relative error of at most 0.025.
Values may be sent and summed in bfloat16 or wider, within the bound.
A program may use at most 64 MiB of HBM per device.

```python
import jax
import jax.numpy as jnp
from jax import lax

D = 2048
FF = 7168
EXPERTS = 4
TOK_DEV = 8
MICRO = 8
LOCAL = 2
SHARDS = 4
LAYERS = 2
TOKENS = 64
CAP = 5
N_EXPERT = 8


def routing_draw(key):
    folded = jax.random.fold_in(key, 7)
    subkeys = jax.random.split(folded, 5)
    blocks = LAYERS * MICRO * N_EXPERT
    hot_expert = jax.random.randint(subkeys[4], (LAYERS * MICRO,), 0, EXPERTS)
    hot_expert = jnp.repeat(hot_expert, N_EXPERT)[:, None]
    priority = jax.vmap(lambda subkey: jax.random.permutation(subkey, TOK_DEV))(jax.random.split(subkeys[2], blocks))
    random_pick = jax.random.randint(subkeys[0], (blocks, TOK_DEV), 0, EXPERTS)
    first_pick = jnp.where(priority < CAP, hot_expert, random_pick)
    offset = jax.random.randint(subkeys[1], (blocks, TOK_DEV), 1, EXPERTS)
    second = (first_pick + offset) % EXPERTS
    chosen = jnp.stack([first_pick, second], axis=-1).astype(jnp.int32)
    prio_pair = jnp.stack([priority * 2, priority * 2 + 1], axis=-1).reshape(blocks, 2 * TOK_DEV)
    flat_ids = chosen.reshape(blocks, 2 * TOK_DEV)
    same_expert = flat_ids[:, :, None] == flat_ids[:, None, :]
    earlier = prio_pair[:, None, :] < prio_pair[:, :, None]
    rank_vals = jnp.sum((same_expert & earlier).astype(jnp.int32), axis=-1)
    drop_flag = (rank_vals >= CAP).astype(jnp.int32)
    spare_slot = jax.random.randint(subkeys[3], (blocks, 2 * TOK_DEV), 0, CAP)
    slot_vals = jnp.where(drop_flag == 1, spare_slot, rank_vals).astype(jnp.int32)
    out_shape = (LAYERS, MICRO, TOKENS, 2)
    return (chosen.reshape(out_shape), slot_vals.reshape(out_shape), drop_flag.reshape(out_shape))


def draw_expert_ids(key, part):
    return routing_draw(key)[0]


def draw_slot_ids(key, part):
    return routing_draw(key)[1]


def draw_dropped(key, part):
    return routing_draw(key)[2]


def shard_levels(stream_key, extent, shards, least, high):
    def one(axis_at, shards_of):
        steps = jax.random.uniform(jax.random.fold_in(jax.random.fold_in(stream_key, 6), axis_at), (shards_of,), jnp.float32, least / len(shards), high / len(shards))
        return jnp.repeat(jnp.exp(steps), extent[axis_at] // shards_of).reshape((-1,) + (1,) * (len(extent) - axis_at - 1))

    level = one(*shards[0])
    for cut in shards[1:]:
        level = level * one(*cut)
    return level


def gaussian(rng, dims, deviation, reach, shards=(), held_as=jnp.bfloat16):
    result = deviation * jax.random.normal(rng, dims, jnp.float32)
    if shards:
        result = result * shard_levels(rng, dims, shards, -0.22, 0.18)
    return jnp.clip(result, -reach, reach).astype(held_as)


def setup_inputs(seed: int = 0) -> dict:
    keys = jax.random.split(jax.random.key(seed), 10)
    tokens = gaussian(keys[0], (MICRO, TOKENS, D), 1.0, 6.0, ((1, 8),))
    norm_gain = jnp.clip(1.0 + 0.18 * jax.random.normal(keys[1], (LAYERS, D), jnp.float32), 0.1, 1.9)
    w_gate = gaussian(keys[2], (2 * LAYERS, D, LOCAL * FF), D ** -0.5, 0.125, ((0, 4), (2, 8)))
    w_up = gaussian(keys[3], (2 * LAYERS, D, LOCAL * FF), D ** -0.5, 0.125, ((0, 4), (2, 8)))
    w_down = gaussian(keys[4], (2 * LAYERS, LOCAL * FF, D), FF ** -0.5, 0.0625, ((0, 4), (1, 8)))
    expert_ids = draw_expert_ids(jax.random.fold_in(keys[9], 71), 0)
    slot_ids = draw_slot_ids(jax.random.fold_in(keys[9], 71), 0)
    dropped = draw_dropped(jax.random.fold_in(keys[9], 71), 0)
    gate_weights = jnp.clip(0.1 + 0.9 * jax.random.uniform(keys[8], (LAYERS, MICRO, TOKENS, 2), jnp.float32) ** shard_levels(keys[8], (LAYERS, MICRO, TOKENS, 2), ((2, 8),), -0.2, 0.2), 0.1, 1.0)
    return dict(tokens=tokens, norm_gain=norm_gain, w_gate=w_gate, w_up=w_up, w_down=w_down, expert_ids=expert_ids, slot_ids=slot_ids, dropped=dropped, gate_weights=gate_weights)


def rms_norm(values, gain_row):
    wide_vals = values.astype(jnp.float32)
    inv_scale = lax.rsqrt(lax.optimization_barrier(jnp.mean(wide_vals * wide_vals, axis=-1, keepdims=True)) + 1e-05)
    return (wide_vals * inv_scale * gain_row).astype(jnp.bfloat16)

def expert_output(rows_in, gate_cols, up_cols, down_rows):
    row_count = rows_in.shape[0]
    gate_vals = jnp.dot(rows_in, gate_cols, preferred_element_type=jnp.float32)
    up_vals = jnp.dot(rows_in, up_cols, preferred_element_type=jnp.float32)
    hidden = (jax.nn.silu(gate_vals) * up_vals).astype(jnp.bfloat16)
    pieces = hidden.reshape(row_count, SHARDS, FF // SHARDS).astype(jnp.float32)
    blocks = down_rows.reshape(SHARDS, FF // SHARDS, D).astype(jnp.float32)
    partial_value = jnp.einsum('rsf,sfd->srd', pieces, blocks).astype(jnp.bfloat16)
    partial_value = lax.optimization_barrier(partial_value)
    return lax.optimization_barrier(jnp.sum(partial_value.astype(jnp.float32), axis=0)).astype(jnp.bfloat16)

def reference(tokens, norm_gain, w_gate, w_up, w_down, expert_ids, slot_ids, dropped, gate_weights):
    slot_limit = EXPERTS * N_EXPERT * CAP
    source = (jnp.arange(TOKENS, dtype=jnp.int32) // TOK_DEV)[:, None]
    gate_all = w_gate.reshape(LAYERS, 2, D, LOCAL * FF)
    up_all = w_up.reshape(LAYERS, 2, D, LOCAL * FF)
    down_all = w_down.reshape(LAYERS, 2, LOCAL * FF, D)

    def one_layer(state, layer_args):
        gain_row, gate_pair, up_pair, down_pair, route_all, slot_all, drop_all, weigh_all = layer_args

        def one_micro(pieces):
            current, route_now, slot_now, drop_now, weigh_now = pieces
            normed = rms_norm(current, gain_row)
            target = route_now * (N_EXPERT * CAP) + source * CAP + slot_now
            target = jnp.where(drop_now == 1, slot_limit, target).astype(jnp.int32)
            buffer = jnp.zeros((slot_limit, D), jnp.bfloat16)
            buffer = buffer.at[target[:, 0]].set(normed, mode='drop')
            buffer = buffer.at[target[:, 1]].set(normed, mode='drop')
            grouped = buffer.reshape(EXPERTS, N_EXPERT * CAP, D)
            outputs = []
            for expert_at in range(EXPERTS):
                half_index = expert_at // LOCAL
                inner_index = expert_at % LOCAL
                low = inner_index * FF
                high = (inner_index + 1) * FF
                outputs.append(expert_output(grouped[expert_at], gate_pair[half_index][:, low:high], up_pair[half_index][:, low:high], down_pair[half_index][low:high]))
            produced = jnp.concatenate(outputs, axis=0)
            clipped = jnp.minimum(target, slot_limit - 1).astype(jnp.int32)
            first_half = current.astype(jnp.float32)
            full_mix = current.astype(jnp.float32)
            for member in range(2):
                picked = produced[clipped[:, member]].astype(jnp.float32)
                weighted = weigh_now[:, member:member + 1] * picked
                kept_mask = drop_now[:, member:member + 1] == 0
                first_kept = kept_mask & (route_now[:, member:member + 1] < LOCAL)
                first_half = first_half + jnp.where(first_kept, weighted, 0.0)
                full_mix = full_mix + jnp.where(kept_mask, weighted, 0.0)
            return (first_half.astype(jnp.bfloat16), full_mix.astype(jnp.bfloat16))
        half_state, new_state = lax.map(one_micro, (state, route_all, slot_all, drop_all, weigh_all))
        return (new_state, jnp.stack([half_state, new_state]))
    final_state, paired = lax.scan(one_layer, tokens, (norm_gain, gate_all, up_all, down_all, expert_ids, slot_ids, dropped, gate_weights))
    return paired.reshape(2 * LAYERS, MICRO, TOKENS, D)
```

```python
import functools

import jax
import jax.numpy as jnp
from jax import lax
from jax.experimental import pallas as pl
from jax.experimental.pallas import tpu as pltpu
from jax.sharding import PartitionSpec as P

CORES = 2
LOCAL = 2
TILE_ROWS = 8


def plan(micro_count, capacity):
    per_chunk = max(1, 16 // capacity)
    later = -(-micro_count // per_chunk) - 1
    sizes = [micro_count - later * per_chunk] + [per_chunk] * later
    chunks, start, before = [], 0, 0
    for size in sizes:
        rows = -(-size * capacity // TILE_ROWS) * TILE_ROWS
        chunks.append((start, size, rows, before))
        start += size
        before += rows
    return chunks, before


def kernel(
    groups, layers, chunks, capacity,
    tok, gain_hbm, ids_hbm, slots_hbm, dropped_hbm, weigh_hbm, gate_hbm, up_hbm, down_hbm,
    out,
    gain, ids, slots, dropped, weigh, gate, up, down, rbuf, sbuf, pbuf, twin, rsum, retbuf, fbuf, whole, cin, hin, xin, hid, vals, cols,
    wsem, tok_sem, small_sem, disp_send, disp_recv, relay_send, twin_send, twin_recv, ret_send, ret_recv,
    next_send, next_recv, part_send, part_recv,
):
    count = len(chunks)
    chips = groups // CORES
    per_expert = chips // LOCAL
    micro_count, tok_rows, model_width = xin.shape
    width = gate.shape[-1]
    section = lax.axis_index("section")
    me = lax.axis_index("expert")
    layer = section // 2
    half = section % 2
    chip = me // CORES
    core = me % CORES
    mine_at = chip // per_expert
    sibling = me + 1 - 2 * core
    inner_layer = layer < layers - 1
    next_layer = lax.rem(layer + 1, layers)
    last_layer = lax.rem(layer - 1 + layers, layers)
    leads = (core == 1) & inner_layer

    def fetch(i):
        src, dst = ((gate_hbm, gate), (up_hbm, up), (down_hbm, down))[i]
        return pltpu.make_async_copy(src.at[0], dst, wsem.at[i])

    def small(i):
        src = (gain_hbm, ids_hbm, slots_hbm, dropped_hbm, weigh_hbm)[i]
        return pltpu.make_async_copy(src, (gain, ids, slots, dropped, weigh)[i], small_sem.at[i])

    def greet():
        barrier = pltpu.get_barrier_semaphore()

        def meet(**where):
            pl.semaphore_signal(barrier, inc=1, device_id=where, device_id_type=pl.DeviceIdType.MESH)

        def meet_layer(other):
            for to in range(2):
                meet(section=2 * other + to)

            @pl.when(core == 1)
            def _():
                for r in range(1, chips):
                    meet(section=2 * other + half, expert=chip_at(r) * CORES + core)

        for r in range(chips - 1, 0, -1):
            meet(expert=chip_at(r) * CORES + core)
        meet(section=2 * layer + 1 - half)

        @pl.when(inner_layer)
        def _():
            meet_layer(next_layer)

        @pl.when(layer > 0)
        def _():
            meet_layer(last_layer)

        meet(expert=sibling)
        beside = jnp.where(inner_layer, 1, 0) + jnp.where(layer > 0, 1, 0)
        pl.semaphore_wait(barrier, chips + 1 + beside * (2 + core * (chips - 1)))

    def load_tokens():
        return pltpu.make_async_copy(tok, xin, tok_sem)

    def span(base, index, size):
        return pl.ds(pl.multiple_of(base + index * size, TILE_ROWS), size)

    def remote(src, dst, send, recv, **where):
        return pltpu.make_async_remote_copy(
            src_ref=src, dst_ref=dst, send_sem=send, recv_sem=recv,
            device_id=where, device_id_type=pl.DeviceIdType.MESH,
        )

    def chip_at(r):
        return lax.rem(chip + r, chips)

    def held(c, place):
        rows, before = chunks[c][2:]
        return rbuf.at[span(before * groups, place, rows)]

    def outgoing(c, which, group):
        rows, before = chunks[c][2:]
        return sbuf.at[which, span(before * LOCAL, group, rows)]

    def direct(c, which, r, to):
        there = chip_at(r)
        place = core * chips + chip
        return remote(
            outgoing(c, which, there // per_expert), held(c, place), disp_send.at[which, c, r],
            disp_recv.at[c, place], section=2 * to + half, expert=there * CORES + core,
        )

    def own_rows(c):
        place = core * chips + chip
        return remote(
            outgoing(c, 0, mine_at), held(c, place), disp_send.at[0, c, 0], disp_recv.at[c, place], expert=sibling
        )

    def relay(c, r):
        place = core * chips + chip_at(r)
        return remote(held(c, place), held(c, place), relay_send.at[c, r], disp_recv.at[c, place], expert=sibling)

    def arrival(c, at_core, at_chip):
        place = at_core * chips + at_chip
        return remote(held(c, place), held(c, place), relay_send.at[c, 0], disp_recv.at[c, place], expert=sibling)

    def per_core(ref, c):
        rows, before = chunks[c][2:]
        return ref.at[pl.ds(before * chips, rows * chips)]

    def to_twin(c):
        rows, before = chunks[c][2:]
        return remote(
            pbuf.at[span(before * groups, 1 - core, rows * chips)], per_core(twin, c),
            twin_send.at[c], twin_recv.at[c], expert=sibling,
        )

    def back(ref, c, at_chip):
        rows, before = chunks[c][2:]
        return ref.at[span(before * chips, at_chip, rows)]

    def giving(c, r):
        there = chip_at(r)
        return remote(
            back(rsum, c, there), back(retbuf, c, chip), ret_send.at[c, r], ret_recv.at[c, chip],
            expert=there * CORES + core,
        )

    def given(c, r):
        there = chip_at(r)
        return remote(
            back(rsum, c, there), back(retbuf, c, there), ret_send.at[c, r], ret_recv.at[c, there],
            expert=there * CORES + core,
        )

    def micros(c):
        return pl.ds(chunks[c][0], chunks[c][1])

    def hand_on(c, to):
        return remote(
            fbuf.at[micros(c)], cin.at[half, micros(c)], next_send.at[to, c], next_recv.at[half, c],
            section=2 * next_layer + to,
        )

    def hand_whole(c):
        return remote(
            whole.at[micros(c)], cin.at[0, micros(c)], next_send.at[0, c], next_recv.at[0, c],
            section=2 * next_layer + half,
        )

    def handed(c, which):
        return remote(
            fbuf.at[micros(c)], cin.at[which, micros(c)], next_send.at[0, c], next_recv.at[which, c],
            section=2 * next_layer,
        )

    def to_partner(c):
        return remote(
            fbuf.at[micros(c)], hin.at[micros(c)], part_send.at[c], part_recv.at[c],
            section=2 * layer + 1 - half,
        )

    def position(c, turn, at_layer):
        start, _, rows, _ = chunks[c]
        at = start + turn
        local = ids[at_layer, at] - half * LOCAL
        owned = (dropped[at_layer, at] == 0) & (local >= 0) & (local < LOCAL)
        return jnp.where(owned, local * rows + turn * capacity + slots[at_layer, at], -1)

    def placed(c, states, at_layer):
        start, size, rows, _ = chunks[c]
        scale = gain[pl.ds(at_layer, 1), :]
        lines = lax.broadcasted_iota(jnp.int32, (LOCAL * rows, tok_rows), 0)
        sent = None
        for turn in range(size):
            current = states[start + turn].astype(jnp.float32)
            inv = lax.rsqrt(jnp.mean(current * current, axis=-1, keepdims=True) + 1e-05)
            normed = (current * inv * scale).astype(jnp.bfloat16)
            pos = position(c, turn, at_layer)
            hot = (lines == pos[0:1, :]) | (lines == pos[1:2, :])
            place = jnp.where(hot, 1.0, 0.0).astype(jnp.bfloat16)
            part = jnp.dot(place, normed, preferred_element_type=jnp.float32)
            sent = part if sent is None else sent + part
        return sent

    def dispatch(c):
        rows, before = chunks[c][2:]
        sent = placed(c, xin, layer)
        sbuf[0, pl.ds(before * LOCAL, LOCAL * rows), :] = sent.astype(jnp.bfloat16)
        own = jnp.where(mine_at == 0, sent[:rows], sent[rows:]).astype(jnp.bfloat16)
        rbuf[span(before * groups, core * chips + chip, rows), :] = own
        for r in range(chips - 1, 0, -1):
            direct(c, 0, r, layer).start()
        own_rows(c).start()

    def dispatch_over(c, which, states, to):
        rows, before = chunks[c][2:]
        sbuf[which, pl.ds(before * LOCAL, LOCAL * rows), :] = placed(c, states, to).astype(jnp.bfloat16)
        for r in range(chips - 1, -1, -1):
            direct(c, which, r, to).start()

    def columns():
        total = micro_count * tok_rows
        for c in range(count):
            for turn in range(chunks[c][1]):
                at = chunks[c][0] + turn
                vals[0, pl.ds(2 * at, 2), :] = position(c, turn, layer).astype(jnp.float32)
                vals[1, pl.ds(2 * at, 2), :] = weigh[layer, at]
        line = lax.broadcasted_iota(jnp.int32, (total, 2 * micro_count), 0)
        lane = lax.broadcasted_iota(jnp.int32, (total, 2 * micro_count), 1)
        small_line = lax.broadcasted_iota(jnp.int32, (total, tok_rows), 0)
        small_lane = lax.broadcasted_iota(jnp.int32, (total, tok_rows), 1)
        own = small_lane < 0
        for m in range(micro_count):
            own = own | (small_line == small_lane + m * tok_rows)
        for k in range(2):
            pick = lane < 0
            for m in range(micro_count):
                pick = pick | ((line >= m * tok_rows) & (line < (m + 1) * tok_rows) & (lane == 2 * m + k))
            pick = jnp.where(pick, 1.0, 0.0)
            for which in range(2):
                wide = jnp.dot(
                    pick, vals[which], precision=lax.Precision.HIGHEST, preferred_element_type=jnp.float32
                )
                cols[2 * k + which] = jnp.sum(jnp.where(own, wide, 0.0), axis=-1, keepdims=True)

    def forward(c):
        @pl.when(core == 1)
        def _():
            arrival(c, core, chip).wait_recv()
            relay(c, 0).start()

        for r in range(1, chips):
            arrival(c, core, chip_at(r)).wait_recv()
            relay(c, r).start()

    def compute(c):
        rows, before = chunks[c][2:]
        lines = rows * groups
        for r in range(chips):
            arrival(c, 1 - core, chip_at(r)).wait_recv()
        if c == 0:
            fetch(0).wait()
            fetch(1).wait()
        wide = 256 if width % 256 == 0 else 128

        def inner(t, carry):
            at = pl.ds(pl.multiple_of(t * wide, wide), wide)
            got = rbuf[pl.ds(before * groups, lines), :]
            g = jnp.dot(got, gate[:, at], preferred_element_type=jnp.float32)
            u = jnp.dot(got, up[:, at], preferred_element_type=jnp.float32)
            hid[pl.ds(0, lines), at] = (g / (1.0 + jnp.exp(-g)) * u).astype(jnp.bfloat16)
            return carry

        lax.fori_loop(0, width // wide, inner, 0, unroll=True)
        if c == 0:
            fetch(2).wait()

        def outer(t, carry):
            at = pl.ds(pl.multiple_of(t * 512, 512), 512)
            pbuf[pl.ds(before * groups, lines), at] = jnp.dot(
                hid[pl.ds(0, lines), :], down[:, at], preferred_element_type=jnp.float32
            ).astype(jnp.bfloat16)
            return carry

        lax.fori_loop(0, model_width // 512, outer, 0, unroll=True)
        to_twin(c).start()

    def pair(c):
        rows, before = chunks[c][2:]
        to_twin(c).wait_recv()
        mine = pbuf[span(before * groups, core, rows * chips), :].astype(jnp.float32)
        other = twin[pl.ds(before * chips, rows * chips), :].astype(jnp.float32)
        rsum[pl.ds(before * chips, rows * chips), :] = (mine + other).astype(jnp.bfloat16)
        for r in range(chips - 1, 0, -1):
            giving(c, r).start()
        retbuf[span(before * chips, chip, rows), :] = rsum[span(before * chips, chip, rows), :]

    def combine(c):
        start, size, rows, before = chunks[c]

        @pl.when((core == 1) & (layer > 0))
        def _():
            handed(c, 0).wait_recv()
            for turn in range(size):
                xin[start + turn] = cin[0, start + turn]

        for r in range(1, chips):
            given(c, r).wait_recv()
        parts = []
        for j in range(LOCAL):
            total = None
            for i in range(per_expert):
                low = before * chips + (j * per_expert + i) * rows
                piece = retbuf[pl.ds(low, rows), :].astype(jnp.float32)
                total = piece if total is None else total + piece
            parts.append(total)
        made = jnp.concatenate(parts, axis=0).astype(jnp.bfloat16)
        tokens = size * tok_rows
        lane = lax.broadcasted_iota(jnp.int32, (tokens, LOCAL * rows), 1).astype(jnp.float32)
        at = pl.ds(start * tok_rows, tokens)
        spread = jnp.zeros((tokens, LOCAL * rows), jnp.float32)
        for k in range(2):
            spread = spread + jnp.where(lane == cols[2 * k, at, :], cols[2 * k + 1, at, :], 0.0)
        coarse = spread.astype(jnp.bfloat16).astype(jnp.float32)
        both = jnp.concatenate([coarse, spread - coarse], axis=0).astype(jnp.bfloat16)
        share = jnp.dot(both, made, preferred_element_type=jnp.float32)
        share = share[:tokens] + share[tokens:]
        for turn in range(size):
            piece = share[turn * tok_rows : (turn + 1) * tok_rows]
            summed = xin[start + turn].astype(jnp.float32) + piece
            fbuf[start + turn] = jnp.where(half == 0, summed, piece).astype(jnp.bfloat16)

        @pl.when(inner_layer & (core == 0))
        def _():
            hand_on(c, 1).start()
            hand_on(c, 0).start()

        @pl.when(leads | ((half == 0) & (layer == layers - 1)))
        def _():
            to_partner(c).start()

        @pl.when(half == 0)
        def _():
            for turn in range(size):
                out[start + turn] = fbuf[start + turn]

    def total(c):
        start, size = chunks[c][:2]
        to_partner(c).wait_recv()
        for turn in range(size):
            at = start + turn
            whole[at] = (hin[at].astype(jnp.float32) + fbuf[at].astype(jnp.float32)).astype(jnp.bfloat16)

    def lead(c):
        @pl.when(leads)
        def _():
            total(c)
            dispatch_over(c, 1, whole, next_layer)
            hand_whole(c).start()

    def finish(c):
        start, size = chunks[c][:2]

        @pl.when((half == 1) & ~leads)
        def _():
            total(c)

        @pl.when(half == 1)
        def _():
            for turn in range(size):
                out[start + turn] = whole[start + turn]

    def first(c):
        if c < count:
            @pl.when((layer == 0) & (core == 0))
            def _():
                dispatch(c)

    def later(c):
        if c < count:
            start, size = chunks[c][:2]

            @pl.when((layer > 0) & (core == 0))
            def _():
                handed(c, 0).wait_recv()
                handed(c, 1).wait_recv()
                for turn in range(size):
                    at = start + turn
                    xin[at] = (cin[0, at].astype(jnp.float32) + cin[1, at].astype(jnp.float32)).astype(jnp.bfloat16)
                dispatch(c)

    helps = (layer == 1) & (core == 1)

    for i in range(5):
        small(i).start()

    @pl.when((layer == 0) | helps)
    def _():
        load_tokens().start()

    greet()
    for i in range(5):
        small(i).wait()

    @pl.when((layer == 0) | helps)
    def _():
        load_tokens().wait()

    for i in range(3):
        fetch(i).start()

    first(0)
    columns()

    @pl.when(helps)
    def _():
        for c in range(count):
            dispatch_over(c, 0, xin, 0)
            for r in range(chips):
                direct(c, 0, r, 0).wait_send()

    later(0)
    forward(0)
    first(1)
    first(2)
    for c in range(count):
        if c >= 1:
            later(c + 1)
        compute(c)
        if c == 0:
            later(1)
        if c >= 2:
            combine(c - 2)
        pair(c)
        first(c + 3)
        if c >= 2:
            lead(c - 2)
        if c + 1 < count:
            forward(c + 1)
    for c in range(max(count - 2, 0), count):
        combine(c)
        lead(c)
    @pl.when((half == 0) & (core == 0) & inner_layer)
    def _():
        for c in range(count):
            to_partner(c).start()

    for c in range(count):
        finish(c)

    for c in range(count):
        to_twin(c).wait_send()
        for r in range(1, chips):
            relay(c, r).wait_send()
            giving(c, r).wait_send()

    @pl.when(core == 0)
    def _():
        for c in range(count):
            own_rows(c).wait_send()
            for r in range(1, chips):
                direct(c, 0, r, layer).wait_send()

    @pl.when(core == 1)
    def _():
        for c in range(count):
            relay(c, 0).wait_send()

    @pl.when(leads)
    def _():
        for c in range(count):
            hand_whole(c).wait_send()
            for r in range(chips):
                direct(c, 1, r, next_layer).wait_send()

    @pl.when(inner_layer & (core == 0))
    def _():
        for c in range(count):
            hand_on(c, 0).wait_send()
            hand_on(c, 1).wait_send()

    @pl.when((half == 0) | leads)
    def _():
        for c in range(count):
            to_partner(c).wait_send()


def on_device(tokens, norm_gain, w_gate, w_up, w_down, expert_ids, slot_ids, dropped, gate_weights):
    groups = lax.axis_size("expert")
    layers = lax.axis_size("section") // 2
    micro_count, tok_rows, model_width = tokens.shape
    width = w_gate.shape[-1]
    capacity = 5 * tok_rows // (4 * LOCAL)
    chunks, total = plan(micro_count, capacity)
    chips = groups // CORES
    count = len(chunks)
    most = max(rows for _, _, rows, _ in chunks)

    def by_choice(value):
        return jnp.transpose(value, (0, 1, 3, 2))

    vm = pl.BlockSpec(memory_space=pltpu.VMEM)
    hb = pl.BlockSpec(memory_space=pl.ANY)
    half16 = jnp.bfloat16
    dma = pltpu.SemaphoreType.DMA
    choices = (layers, micro_count, 2, tok_rows)
    state = (micro_count, tok_rows, model_width)
    made = pl.pallas_call(
        functools.partial(kernel, groups, layers, chunks, capacity),
        out_shape=jax.ShapeDtypeStruct(state, half16),
        in_specs=[hb] * 9,
        out_specs=vm,
        scratch_shapes=[
            pltpu.VMEM(norm_gain.shape, jnp.float32),
            pltpu.VMEM(choices, jnp.int32),
            pltpu.VMEM(choices, jnp.int32),
            pltpu.VMEM(choices, jnp.int32),
            pltpu.VMEM(choices, jnp.float32),
            pltpu.VMEM((model_width, width), half16),
            pltpu.VMEM((model_width, width), half16),
            pltpu.VMEM((width, model_width), half16),
            pltpu.VMEM((total * groups, model_width), half16),
            pltpu.VMEM((2, total * LOCAL, model_width), half16),
            pltpu.VMEM((total * groups, model_width), half16),
            pltpu.VMEM((total * chips, model_width), half16),
            pltpu.VMEM((total * chips, model_width), half16),
            pltpu.VMEM((total * chips, model_width), half16),
            pltpu.VMEM(state, half16),
            pltpu.VMEM(state, half16),
            pltpu.VMEM((2,) + state, half16),
            pltpu.VMEM(state, half16),
            pltpu.VMEM(state, half16),
            pltpu.VMEM((groups * most, width), half16),
            pltpu.VMEM((2, 2 * micro_count, tok_rows), jnp.float32),
            pltpu.VMEM((4, micro_count * tok_rows, 1), jnp.float32),
            dma((3,)),
            dma,
            dma((5,)),
            dma((2, count, chips)),
            dma((count, groups)),
            dma((count, chips)),
            dma((count,)),
            dma((count,)),
            dma((count, chips)),
            dma((count, chips)),
            dma((2, count)),
            dma((2, count)),
            dma((count,)),
            dma((count,)),
        ],
        compiler_params=pltpu.CompilerParams(
            collective_id=0, has_side_effects=True, vmem_limit_bytes=58 * 1024 * 1024
        ),
    )(
        tokens, norm_gain, by_choice(expert_ids), by_choice(slot_ids), by_choice(dropped), by_choice(gate_weights),
        w_gate, w_up, w_down,
    )
    return made[None]


def solution(mesh):
    return jax.shard_map(
        on_device,
        mesh=mesh,
        in_specs=(
            P(None, "expert", None),
            P(),
            P("section", None, "expert"),
            P("section", None, "expert"),
            P("section", "expert", None),
            P(None, None, "expert", None),
            P(None, None, "expert", None),
            P(None, None, "expert", None),
            P(None, None, "expert", None),
        ),
        out_specs=P("section", None, "expert", None),
        check_vma=False,
    )
```

```python
import functools

import jax
import jax.numpy as jnp
from jax import lax
from jax.experimental import pallas as pl
from jax.experimental.pallas import tpu as pltpu
from jax.sharding import PartitionSpec as P

CORES = 2
LOCAL = 2
TILE_ROWS = 8
DUE = ({2: (0,)}, {})


def plan(micro_count, capacity):
    per_chunk = max(1, 16 // capacity)
    later = -(-micro_count // per_chunk) - 1
    sizes = [micro_count - later * per_chunk] + [per_chunk] * later
    chunks, start, before = [], 0, 0
    for size in sizes:
        rows = -(-size * capacity // TILE_ROWS) * TILE_ROWS
        chunks.append((start, size, rows, before))
        start += size
        before += rows
    return chunks, before


def kernel(
    groups, layers, chunks, capacity,
    tok, gain_hbm, ids_hbm, slots_hbm, dropped_hbm, weigh_hbm, gate_hbm, up_hbm, down_hbm,
    out,
    gain, ids, slots, dropped, weigh, gate, up, down, rbuf, sbuf, pbuf, twin, rsum, retbuf, fbuf, whole, cin, hin, xin, hid, vals, cols,
    wsem, tok_sem, small_sem, disp_send, disp_recv, relay_send, twin_send, twin_recv, ret_send, ret_recv,
    next_send, next_recv, part_send, part_recv,
):
    count = len(chunks)
    chips = groups // CORES
    per_expert = chips // LOCAL
    micro_count, tok_rows, model_width = xin.shape
    width = gate.shape[-1]
    section = lax.axis_index("section")
    me = lax.axis_index("expert")
    layer = section // 2
    half = section % 2
    chip = me // CORES
    core = me % CORES
    mine_at = chip // per_expert
    sibling = me + 1 - 2 * core
    inner_layer = layer < layers - 1
    next_layer = lax.rem(layer + 1, layers)
    last_layer = lax.rem(layer - 1 + layers, layers)
    helps = (layer == 1) & (core == 1)

    def leads(c):
        return inner_layer if c >= 1 else layer < 0

    def places_own(c):
        own = (layer == 0) & (core == 0)
        return own | (layer > 0) if c == 0 else own


    def fetch(i):
        src, dst = ((gate_hbm, gate), (up_hbm, up), (down_hbm, down))[i]
        return pltpu.make_async_copy(src.at[0], dst, wsem.at[i])

    def small(i):
        src = (gain_hbm, ids_hbm, slots_hbm, dropped_hbm, weigh_hbm)[i]
        return pltpu.make_async_copy(src, (gain, ids, slots, dropped, weigh)[i], small_sem.at[i])

    def greet():
        barrier = pltpu.get_barrier_semaphore()

        def meet(**where):
            pl.semaphore_signal(barrier, inc=1, device_id=where, device_id_type=pl.DeviceIdType.MESH)

        def meet_layer(other):
            for to in range(2):
                meet(section=2 * other + to)

            for r in range(1, chips):
                meet(section=2 * other + half, expert=chip_at(r) * CORES + core)

        for r in range(chips - 1, 0, -1):
            meet(expert=chip_at(r) * CORES + core)
        meet(section=2 * layer + 1 - half)

        @pl.when(inner_layer)
        def _():
            meet_layer(next_layer)

        @pl.when(layer > 0)
        def _():
            meet_layer(last_layer)

        meet(expert=sibling)
        beside = jnp.where(inner_layer, 1, 0) + jnp.where(layer > 0, 1, 0)
        pl.semaphore_wait(barrier, chips + 1 + beside * (chips + 1))

    def load_tokens():
        return pltpu.make_async_copy(tok, xin, tok_sem)

    def span(base, index, size):
        return pl.ds(pl.multiple_of(base + index * size, TILE_ROWS), size)

    def remote(src, dst, send, recv, **where):
        return pltpu.make_async_remote_copy(
            src_ref=src, dst_ref=dst, send_sem=send, recv_sem=recv,
            device_id=where, device_id_type=pl.DeviceIdType.MESH,
        )

    def chip_at(r):
        return lax.rem(chip + r, chips)

    def held(c, place):
        rows, before = chunks[c][2:]
        return rbuf.at[span(before * groups, place, rows)]

    def outgoing(c, which, group):
        rows, before = chunks[c][2:]
        return sbuf.at[which, span(before * LOCAL, group, rows)]

    def direct(c, which, r, to):
        there = chip_at(r)
        place = core * chips + chip
        return remote(
            outgoing(c, which, there // per_expert), held(c, place), disp_send.at[which, c, r],
            disp_recv.at[c, place], section=2 * to + half, expert=there * CORES + core,
        )

    def own_rows(c):
        place = core * chips + chip
        return remote(
            outgoing(c, 0, mine_at), held(c, place), disp_send.at[0, c, 0], disp_recv.at[c, place], expert=sibling
        )

    def relay(c, r):
        place = core * chips + chip_at(r)
        return remote(held(c, place), held(c, place), relay_send.at[c, r], disp_recv.at[c, place], expert=sibling)

    def arrival(c, at_core, at_chip):
        place = at_core * chips + at_chip
        return remote(held(c, place), held(c, place), relay_send.at[c, 0], disp_recv.at[c, place], expert=sibling)

    def per_core(ref, c):
        rows, before = chunks[c][2:]
        return ref.at[pl.ds(before * chips, rows * chips)]

    def to_twin(c):
        rows, before = chunks[c][2:]
        return remote(
            pbuf.at[span(before * groups, 1 - core, rows * chips)], per_core(twin, c),
            twin_send.at[c], twin_recv.at[c], expert=sibling,
        )

    def back(ref, c, at_chip):
        rows, before = chunks[c][2:]
        return ref.at[span(before * chips, at_chip, rows)]

    def giving(c, r):
        there = chip_at(r)
        return remote(
            back(rsum, c, there), back(retbuf, c, chip), ret_send.at[c, r], ret_recv.at[c, chip],
            expert=there * CORES + core,
        )

    def given(c, r):
        there = chip_at(r)
        return remote(
            back(rsum, c, there), back(retbuf, c, there), ret_send.at[c, r], ret_recv.at[c, there],
            expert=there * CORES + core,
        )

    def micros(c):
        return pl.ds(chunks[c][0], chunks[c][1])

    def hand_on(c, to):
        return remote(
            fbuf.at[micros(c)], cin.at[half, micros(c)], next_send.at[to, c], next_recv.at[half, c],
            section=2 * next_layer + to,
        )

    def hand_whole(c):
        return remote(
            whole.at[micros(c)], cin.at[0, micros(c)], next_send.at[0, c], next_recv.at[0, c],
            section=2 * next_layer + half,
        )

    def handed(c, which):
        return remote(
            fbuf.at[micros(c)], cin.at[which, micros(c)], next_send.at[0, c], next_recv.at[which, c],
            section=2 * next_layer,
        )

    def to_partner(c):
        return remote(
            fbuf.at[micros(c)], hin.at[micros(c)], part_send.at[c], part_recv.at[c],
            section=2 * layer + 1 - half,
        )

    def position(c, turn, at_layer):
        start, _, rows, _ = chunks[c]
        at = start + turn
        local = ids[at_layer, at] - half * LOCAL
        owned = (dropped[at_layer, at] == 0) & (local >= 0) & (local < LOCAL)
        return jnp.where(owned, local * rows + turn * capacity + slots[at_layer, at], -1)

    def placed(c, states, at_layer):
        start, size, rows, _ = chunks[c]
        scale = gain[pl.ds(at_layer, 1), :]
        lines = lax.broadcasted_iota(jnp.int32, (LOCAL * rows, tok_rows), 0)
        sent = None
        for turn in range(size):
            current = states[start + turn].astype(jnp.float32)
            inv = lax.rsqrt(jnp.mean(current * current, axis=-1, keepdims=True) + 1e-05)
            normed = (current * inv * scale).astype(jnp.bfloat16)
            pos = position(c, turn, at_layer)
            hot = (lines == pos[0:1, :]) | (lines == pos[1:2, :])
            place = jnp.where(hot, 1.0, 0.0).astype(jnp.bfloat16)
            part = jnp.dot(place, normed, preferred_element_type=jnp.float32)
            sent = part if sent is None else sent + part
        return sent

    def dispatch(c):
        rows, before = chunks[c][2:]
        sent = placed(c, xin, layer)
        sbuf[0, pl.ds(before * LOCAL, LOCAL * rows), :] = sent.astype(jnp.bfloat16)
        own = jnp.where(mine_at == 0, sent[:rows], sent[rows:]).astype(jnp.bfloat16)
        rbuf[span(before * groups, core * chips + chip, rows), :] = own
        for r in range(chips - 1, 0, -1):
            direct(c, 0, r, layer).start()
        own_rows(c).start()

    def dispatch_over(c, which, states, to):
        rows, before = chunks[c][2:]
        sbuf[which, pl.ds(before * LOCAL, LOCAL * rows), :] = placed(c, states, to).astype(jnp.bfloat16)
        for r in range(chips - 1, -1, -1):
            direct(c, which, r, to).start()

    def columns():
        total = micro_count * tok_rows
        for c in range(count):
            for turn in range(chunks[c][1]):
                at = chunks[c][0] + turn
                vals[0, pl.ds(2 * at, 2), :] = position(c, turn, layer).astype(jnp.float32)
                vals[1, pl.ds(2 * at, 2), :] = weigh[layer, at]
        line = lax.broadcasted_iota(jnp.int32, (total, 2 * micro_count), 0)
        lane = lax.broadcasted_iota(jnp.int32, (total, 2 * micro_count), 1)
        small_line = lax.broadcasted_iota(jnp.int32, (total, tok_rows), 0)
        small_lane = lax.broadcasted_iota(jnp.int32, (total, tok_rows), 1)
        own = small_lane < 0
        for m in range(micro_count):
            own = own | (small_line == small_lane + m * tok_rows)
        for k in range(2):
            pick = lane < 0
            for m in range(micro_count):
                pick = pick | ((line >= m * tok_rows) & (line < (m + 1) * tok_rows) & (lane == 2 * m + k))
            pick = jnp.where(pick, 1.0, 0.0)
            for which in range(2):
                wide = jnp.dot(
                    pick, vals[which], precision=lax.Precision.HIGHEST, preferred_element_type=jnp.float32
                )
                cols[2 * k + which] = jnp.sum(jnp.where(own, wide, 0.0), axis=-1, keepdims=True)

    def forward(c):
        @pl.when(~places_own(c))
        def _():
            arrival(c, core, chip).wait_recv()
            relay(c, 0).start()

        for r in range(1, chips):
            arrival(c, core, chip_at(r)).wait_recv()
            relay(c, r).start()

    def compute(c):
        rows, before = chunks[c][2:]
        lines = rows * groups
        for r in range(chips):
            arrival(c, 1 - core, chip_at(r)).wait_recv()
        if c == 0:
            fetch(0).wait()
            fetch(1).wait()
        wide = 256 if width % 256 == 0 else 128

        def inner(t, carry):
            at = pl.ds(pl.multiple_of(t * wide, wide), wide)
            got = rbuf[pl.ds(before * groups, lines), :]
            g = jnp.dot(got, gate[:, at], preferred_element_type=jnp.float32)
            u = jnp.dot(got, up[:, at], preferred_element_type=jnp.float32)
            hid[pl.ds(0, lines), at] = (g / (1.0 + jnp.exp(-g)) * u).astype(jnp.bfloat16)
            return carry

        lax.fori_loop(0, width // wide, inner, 0, unroll=True)
        if c == 0:
            fetch(2).wait()

        def outer(t, carry):
            at = pl.ds(pl.multiple_of(t * 512, 512), 512)
            pbuf[pl.ds(before * groups, lines), at] = jnp.dot(
                hid[pl.ds(0, lines), :], down[:, at], preferred_element_type=jnp.float32
            ).astype(jnp.bfloat16)
            return carry

        lax.fori_loop(0, model_width // 512, outer, 0, unroll=True)
        to_twin(c).start()

    def pair(c):
        rows, before = chunks[c][2:]
        to_twin(c).wait_recv()
        mine = pbuf[span(before * groups, core, rows * chips), :].astype(jnp.float32)
        other = twin[pl.ds(before * chips, rows * chips), :].astype(jnp.float32)
        rsum[pl.ds(before * chips, rows * chips), :] = (mine + other).astype(jnp.bfloat16)
        for r in range(chips - 1, 0, -1):
            giving(c, r).start()
        retbuf[span(before * chips, chip, rows), :] = rsum[span(before * chips, chip, rows), :]

    def combine(c):
        start, size, rows, before = chunks[c]

        if c >= 1:
            @pl.when(layer > 0)
            def _():
                handed(c, 0).wait_recv()
                for turn in range(size):
                    xin[start + turn] = cin[0, start + turn]

        for r in range(1, chips):
            given(c, r).wait_recv()
        parts = []
        for j in range(LOCAL):
            total = None
            for i in range(per_expert):
                low = before * chips + (j * per_expert + i) * rows
                piece = retbuf[pl.ds(low, rows), :].astype(jnp.float32)
                total = piece if total is None else total + piece
            parts.append(total)
        made = jnp.concatenate(parts, axis=0).astype(jnp.bfloat16)
        tokens = size * tok_rows
        lane = lax.broadcasted_iota(jnp.int32, (tokens, LOCAL * rows), 1).astype(jnp.float32)
        at = pl.ds(start * tok_rows, tokens)
        spread = jnp.zeros((tokens, LOCAL * rows), jnp.float32)
        for k in range(2):
            spread = spread + jnp.where(lane == cols[2 * k, at, :], cols[2 * k + 1, at, :], 0.0)
        coarse = spread.astype(jnp.bfloat16).astype(jnp.float32)
        both = jnp.concatenate([coarse, spread - coarse], axis=0).astype(jnp.bfloat16)
        share = jnp.dot(both, made, preferred_element_type=jnp.float32)
        share = share[:tokens] + share[tokens:]
        for turn in range(size):
            piece = share[turn * tok_rows : (turn + 1) * tok_rows]
            summed = xin[start + turn].astype(jnp.float32) + piece
            fbuf[start + turn] = jnp.where(half == 0, summed, piece).astype(jnp.bfloat16)

        if c == 0:
            @pl.when(inner_layer)
            def _():
                hand_on(c, 1).start()
                hand_on(c, 0).start()

        @pl.when(leads(c) | ((half == 0) & (layer == layers - 1)))
        def _():
            to_partner(c).start()

        @pl.when(half == 0)
        def _():
            for turn in range(size):
                out[start + turn] = fbuf[start + turn]

    def total(c):
        start, size = chunks[c][:2]
        to_partner(c).wait_recv()
        for turn in range(size):
            at = start + turn
            whole[at] = (hin[at].astype(jnp.float32) + fbuf[at].astype(jnp.float32)).astype(jnp.bfloat16)

    def lead(c):
        @pl.when(leads(c))
        def _():
            total(c)
            dispatch_over(c, 1, whole, next_layer)
            hand_whole(c).start()

    def finish(c):
        start, size = chunks[c][:2]

        @pl.when((half == 1) & ~leads(c))
        def _():
            total(c)

        @pl.when(half == 1)
        def _():
            for turn in range(size):
                out[start + turn] = whole[start + turn]

    def first(c):
        if c < count:
            @pl.when((layer == 0) & (core == 0))
            def _():
                dispatch(c)

    def later(c):
        if c < count:
            start, size = chunks[c][:2]

            @pl.when(layer > 0)
            def _():
                handed(c, 0).wait_recv()
                handed(c, 1).wait_recv()
                for turn in range(size):
                    at = start + turn
                    xin[at] = (cin[0, at].astype(jnp.float32) + cin[1, at].astype(jnp.float32)).astype(jnp.bfloat16)
                dispatch(c)

    for i in range(5):
        small(i).start()

    @pl.when((layer == 0) | helps)
    def _():
        load_tokens().start()

    greet()
    for i in range(5):
        small(i).wait()

    @pl.when((layer == 0) | helps)
    def _():
        load_tokens().wait()

    for i in range(3):
        fetch(i).start()

    first(0)
    columns()

    @pl.when(helps)
    def _():
        for c in range(count):
            dispatch_over(c, 0, xin, 0)
            for r in range(chips):
                direct(c, 0, r, 0).wait_send()

    later(0)
    forward(0)
    first(1)
    first(2)
    early, late = DUE
    done = []
    for c in range(count):
        compute(c)
        for other in early.get(c, ()):
            combine(other)
        pair(c)
        first(c + 3)
        for other in late.get(c, ()):
            combine(other)
        for other in early.get(c, ()) + late.get(c, ()):
            lead(other)
            done.append(other)
        if c + 1 < count:
            forward(c + 1)
    for c in range(count):
        if c not in done:
            combine(c)
            lead(c)

    @pl.when((half == 0) & inner_layer)
    def _():
        to_partner(0).start()

    for c in range(count):
        finish(c)

    for c in range(count):
        to_twin(c).wait_send()
        for r in range(1, chips):
            relay(c, r).wait_send()
            giving(c, r).wait_send()

    for c in range(count):
        @pl.when(places_own(c))
        def _():
            own_rows(c).wait_send()
            for r in range(1, chips):
                direct(c, 0, r, layer).wait_send()

        @pl.when(~places_own(c))
        def _():
            relay(c, 0).wait_send()

        @pl.when(leads(c))
        def _():
            hand_whole(c).wait_send()
            for r in range(chips):
                direct(c, 1, r, next_layer).wait_send()

        @pl.when((half == 0) | leads(c))
        def _():
            to_partner(c).wait_send()

    @pl.when(inner_layer)
    def _():
        hand_on(0, 0).wait_send()
        hand_on(0, 1).wait_send()


def on_device(tokens, norm_gain, w_gate, w_up, w_down, expert_ids, slot_ids, dropped, gate_weights):
    groups = lax.axis_size("expert")
    layers = lax.axis_size("section") // 2
    micro_count, tok_rows, model_width = tokens.shape
    width = w_gate.shape[-1]
    capacity = 5 * tok_rows // (4 * LOCAL)
    chunks, total = plan(micro_count, capacity)
    chips = groups // CORES
    count = len(chunks)
    most = max(rows for _, _, rows, _ in chunks)

    def by_choice(value):
        return jnp.transpose(value, (0, 1, 3, 2))

    vm = pl.BlockSpec(memory_space=pltpu.VMEM)
    hb = pl.BlockSpec(memory_space=pl.ANY)
    half16 = jnp.bfloat16
    dma = pltpu.SemaphoreType.DMA
    choices = (layers, micro_count, 2, tok_rows)
    state = (micro_count, tok_rows, model_width)
    made = pl.pallas_call(
        functools.partial(kernel, groups, layers, chunks, capacity),
        out_shape=jax.ShapeDtypeStruct(state, half16),
        in_specs=[hb] * 9,
        out_specs=vm,
        scratch_shapes=[
            pltpu.VMEM(norm_gain.shape, jnp.float32),
            pltpu.VMEM(choices, jnp.int32),
            pltpu.VMEM(choices, jnp.int32),
            pltpu.VMEM(choices, jnp.int32),
            pltpu.VMEM(choices, jnp.float32),
            pltpu.VMEM((model_width, width), half16),
            pltpu.VMEM((model_width, width), half16),
            pltpu.VMEM((width, model_width), half16),
            pltpu.VMEM((total * groups, model_width), half16),
            pltpu.VMEM((2, total * LOCAL, model_width), half16),
            pltpu.VMEM((total * groups, model_width), half16),
            pltpu.VMEM((total * chips, model_width), half16),
            pltpu.VMEM((total * chips, model_width), half16),
            pltpu.VMEM((total * chips, model_width), half16),
            pltpu.VMEM(state, half16),
            pltpu.VMEM(state, half16),
            pltpu.VMEM((2,) + state, half16),
            pltpu.VMEM(state, half16),
            pltpu.VMEM(state, half16),
            pltpu.VMEM((groups * most, width), half16),
            pltpu.VMEM((2, 2 * micro_count, tok_rows), jnp.float32),
            pltpu.VMEM((4, micro_count * tok_rows, 1), jnp.float32),
            dma((3,)),
            dma,
            dma((5,)),
            dma((2, count, chips)),
            dma((count, groups)),
            dma((count, chips)),
            dma((count,)),
            dma((count,)),
            dma((count, chips)),
            dma((count, chips)),
            dma((2, count)),
            dma((2, count)),
            dma((count,)),
            dma((count,)),
        ],
        compiler_params=pltpu.CompilerParams(
            collective_id=0, has_side_effects=True, vmem_limit_bytes=58 * 1024 * 1024
        ),
    )(
        tokens, norm_gain, by_choice(expert_ids), by_choice(slot_ids), by_choice(dropped), by_choice(gate_weights),
        w_gate, w_up, w_down,
    )
    return made[None]


def solution(mesh):
    return jax.shard_map(
        on_device,
        mesh=mesh,
        in_specs=(
            P(None, "expert", None),
            P(),
            P("section", None, "expert"),
            P("section", None, "expert"),
            P("section", "expert", None),
            P(None, None, "expert", None),
            P(None, None, "expert", None),
            P(None, None, "expert", None),
            P(None, None, "expert", None),
        ),
        out_specs=P("section", None, "expert", None),
        check_vma=False,
    )
```

```python
import functools

import jax
import jax.numpy as jnp
from jax import lax
from jax.experimental import pallas as pl
from jax.experimental.pallas import tpu as pltpu
from jax.sharding import PartitionSpec as P

CORES = 2
LOCAL = 2
TILE_ROWS = 8
DUE = ({2: (0,)}, {})


def plan(micro_count, capacity):
    per_chunk = max(1, 16 // capacity)
    later = -(-micro_count // per_chunk) - 1
    sizes = [micro_count - later * per_chunk] + [per_chunk] * later
    chunks, start, before = [], 0, 0
    for size in sizes:
        rows = -(-size * capacity // TILE_ROWS) * TILE_ROWS
        chunks.append((start, size, rows, before))
        start += size
        before += rows
    return chunks, before


def kernel(
    groups, layers, chunks, capacity,
    tok, gain_hbm, ids_hbm, slots_hbm, dropped_hbm, weigh_hbm, gate_hbm, up_hbm, down_hbm,
    out,
    gain, ids, slots, dropped, weigh, gate, up, down, rbuf, sbuf, pbuf, twin, rsum, retbuf, fbuf, whole, cin, hin, xin, hid, vals, cols,
    wsem, tok_sem, small_sem, disp_send, disp_recv, relay_send, twin_send, twin_recv, ret_send, ret_recv,
    next_send, next_recv, part_send, part_recv,
):
    count = len(chunks)
    chips = groups // CORES
    per_expert = chips // LOCAL
    micro_count, tok_rows, model_width = xin.shape
    width = gate.shape[-1]
    section = lax.axis_index("section")
    me = lax.axis_index("expert")
    layer = section // 2
    half = section % 2
    chip = me // CORES
    core = me % CORES
    mine_at = chip // per_expert
    sibling = me + 1 - 2 * core
    inner_layer = layer < layers - 1
    next_layer = lax.rem(layer + 1, layers)
    last_layer = lax.rem(layer - 1 + layers, layers)
    def leads(c):
        return inner_layer if c >= 1 else layer < 0

    def helps(c):
        return layer == 1 if c >= 1 else (layer == 1) & (core == 1)

    def places_own(c):
        return layer < 0 if c >= 1 else (layer > 0) | (core == 0)

    def fetch(i):
        src, dst = ((gate_hbm, gate), (up_hbm, up), (down_hbm, down))[i]
        return pltpu.make_async_copy(src.at[0], dst, wsem.at[i])

    def small(i):
        src = (gain_hbm, ids_hbm, slots_hbm, dropped_hbm, weigh_hbm)[i]
        return pltpu.make_async_copy(src, (gain, ids, slots, dropped, weigh)[i], small_sem.at[i])

    def greet():
        barrier = pltpu.get_barrier_semaphore()

        def meet(**where):
            pl.semaphore_signal(barrier, inc=1, device_id=where, device_id_type=pl.DeviceIdType.MESH)

        def meet_layer(other):
            for to in range(2):
                meet(section=2 * other + to)

            for r in range(1, chips):
                meet(section=2 * other + half, expert=chip_at(r) * CORES + core)

        for r in range(chips - 1, 0, -1):
            meet(expert=chip_at(r) * CORES + core)
        meet(section=2 * layer + 1 - half)

        @pl.when(inner_layer)
        def _():
            meet_layer(next_layer)

        @pl.when(layer > 0)
        def _():
            meet_layer(last_layer)

        meet(expert=sibling)
        beside = jnp.where(inner_layer, 1, 0) + jnp.where(layer > 0, 1, 0)
        pl.semaphore_wait(barrier, chips + 1 + beside * (chips + 1))

    def load_tokens():
        return pltpu.make_async_copy(tok, xin, tok_sem)

    def span(base, index, size):
        return pl.ds(pl.multiple_of(base + index * size, TILE_ROWS), size)

    def remote(src, dst, send, recv, **where):
        return pltpu.make_async_remote_copy(
            src_ref=src, dst_ref=dst, send_sem=send, recv_sem=recv,
            device_id=where, device_id_type=pl.DeviceIdType.MESH,
        )

    def chip_at(r):
        return lax.rem(chip + r, chips)

    def held(c, place):
        rows, before = chunks[c][2:]
        return rbuf.at[span(before * groups, place, rows)]

    def outgoing(c, which, group):
        rows, before = chunks[c][2:]
        return sbuf.at[which, span(before * LOCAL, group, rows)]

    def direct(c, which, r, to):
        there = chip_at(r)
        place = core * chips + chip
        return remote(
            outgoing(c, which, there // per_expert), held(c, place), disp_send.at[which, c, r],
            disp_recv.at[c, place], section=2 * to + half, expert=there * CORES + core,
        )

    def own_rows(c):
        place = core * chips + chip
        return remote(
            outgoing(c, 0, mine_at), held(c, place), disp_send.at[0, c, 0], disp_recv.at[c, place], expert=sibling
        )

    def relay(c, r):
        place = core * chips + chip_at(r)
        return remote(held(c, place), held(c, place), relay_send.at[c, r], disp_recv.at[c, place], expert=sibling)

    def arrival(c, at_core, at_chip):
        place = at_core * chips + at_chip
        return remote(held(c, place), held(c, place), relay_send.at[c, 0], disp_recv.at[c, place], expert=sibling)

    def per_core(ref, c):
        rows, before = chunks[c][2:]
        return ref.at[pl.ds(before * chips, rows * chips)]

    def to_twin(c):
        rows, before = chunks[c][2:]
        return remote(
            pbuf.at[span(before * groups, 1 - core, rows * chips)], per_core(twin, c),
            twin_send.at[c], twin_recv.at[c], expert=sibling,
        )

    def back(ref, c, at_chip):
        rows, before = chunks[c][2:]
        return ref.at[span(before * chips, at_chip, rows)]

    def giving(c, r):
        there = chip_at(r)
        return remote(
            back(rsum, c, there), back(retbuf, c, chip), ret_send.at[c, r], ret_recv.at[c, chip],
            expert=there * CORES + core,
        )

    def given(c, r):
        there = chip_at(r)
        return remote(
            back(rsum, c, there), back(retbuf, c, there), ret_send.at[c, r], ret_recv.at[c, there],
            expert=there * CORES + core,
        )

    def micros(c):
        return pl.ds(chunks[c][0], chunks[c][1])

    def hand_on(c, to):
        return remote(
            fbuf.at[micros(c)], cin.at[half, micros(c)], next_send.at[to, c], next_recv.at[half, c],
            section=2 * next_layer + to,
        )

    def hand_whole(c):
        return remote(
            whole.at[micros(c)], cin.at[0, micros(c)], next_send.at[0, c], next_recv.at[0, c],
            section=2 * next_layer + half,
        )

    def handed(c, which):
        return remote(
            fbuf.at[micros(c)], cin.at[which, micros(c)], next_send.at[0, c], next_recv.at[which, c],
            section=2 * next_layer,
        )

    def to_partner(c):
        return remote(
            fbuf.at[micros(c)], hin.at[micros(c)], part_send.at[c], part_recv.at[c],
            section=2 * layer + 1 - half,
        )

    def position(c, turn, at_layer):
        start, _, rows, _ = chunks[c]
        at = start + turn
        local = ids[at_layer, at] - half * LOCAL
        owned = (dropped[at_layer, at] == 0) & (local >= 0) & (local < LOCAL)
        return jnp.where(owned, local * rows + turn * capacity + slots[at_layer, at], -1)

    def placed(c, states, at_layer):
        start, size, rows, _ = chunks[c]
        scale = gain[pl.ds(at_layer, 1), :]
        lines = lax.broadcasted_iota(jnp.int32, (LOCAL * rows, tok_rows), 0)
        sent = None
        for turn in range(size):
            current = states[start + turn].astype(jnp.float32)
            inv = lax.rsqrt(jnp.mean(current * current, axis=-1, keepdims=True) + 1e-05)
            normed = (current * inv * scale).astype(jnp.bfloat16)
            pos = position(c, turn, at_layer)
            hot = (lines == pos[0:1, :]) | (lines == pos[1:2, :])
            place = jnp.where(hot, 1.0, 0.0).astype(jnp.bfloat16)
            part = jnp.dot(place, normed, preferred_element_type=jnp.float32)
            sent = part if sent is None else sent + part
        return sent

    def dispatch(c):
        rows, before = chunks[c][2:]
        sent = placed(c, xin, layer)
        sbuf[0, pl.ds(before * LOCAL, LOCAL * rows), :] = sent.astype(jnp.bfloat16)
        own = jnp.where(mine_at == 0, sent[:rows], sent[rows:]).astype(jnp.bfloat16)
        rbuf[span(before * groups, core * chips + chip, rows), :] = own
        for r in range(chips - 1, 0, -1):
            direct(c, 0, r, layer).start()
        own_rows(c).start()

    def dispatch_over(c, which, states, to):
        rows, before = chunks[c][2:]
        sbuf[which, pl.ds(before * LOCAL, LOCAL * rows), :] = placed(c, states, to).astype(jnp.bfloat16)
        for r in range(chips - 1, -1, -1):
            direct(c, which, r, to).start()

    def columns():
        total = micro_count * tok_rows
        for c in range(count):
            for turn in range(chunks[c][1]):
                at = chunks[c][0] + turn
                vals[0, pl.ds(2 * at, 2), :] = position(c, turn, layer).astype(jnp.float32)
                vals[1, pl.ds(2 * at, 2), :] = weigh[layer, at]
        line = lax.broadcasted_iota(jnp.int32, (total, 2 * micro_count), 0)
        lane = lax.broadcasted_iota(jnp.int32, (total, 2 * micro_count), 1)
        small_line = lax.broadcasted_iota(jnp.int32, (total, tok_rows), 0)
        small_lane = lax.broadcasted_iota(jnp.int32, (total, tok_rows), 1)
        own = small_lane < 0
        for m in range(micro_count):
            own = own | (small_line == small_lane + m * tok_rows)
        for k in range(2):
            pick = lane < 0
            for m in range(micro_count):
                pick = pick | ((line >= m * tok_rows) & (line < (m + 1) * tok_rows) & (lane == 2 * m + k))
            pick = jnp.where(pick, 1.0, 0.0)
            for which in range(2):
                wide = jnp.dot(
                    pick, vals[which], precision=lax.Precision.HIGHEST, preferred_element_type=jnp.float32
                )
                cols[2 * k + which] = jnp.sum(jnp.where(own, wide, 0.0), axis=-1, keepdims=True)

    def forward(c):
        @pl.when(~places_own(c))
        def _():
            arrival(c, core, chip).wait_recv()
            relay(c, 0).start()

        for r in range(1, chips):
            arrival(c, core, chip_at(r)).wait_recv()
            relay(c, r).start()

    def compute(c):
        rows, before = chunks[c][2:]
        lines = rows * groups
        for r in range(chips):
            arrival(c, 1 - core, chip_at(r)).wait_recv()
        if c == 0:
            fetch(0).wait()
            fetch(1).wait()
        wide = 256 if width % 256 == 0 else 128

        def inner(t, carry):
            at = pl.ds(pl.multiple_of(t * wide, wide), wide)
            got = rbuf[pl.ds(before * groups, lines), :]
            g = jnp.dot(got, gate[:, at], preferred_element_type=jnp.float32)
            u = jnp.dot(got, up[:, at], preferred_element_type=jnp.float32)
            hid[pl.ds(0, lines), at] = (g / (1.0 + jnp.exp(-g)) * u).astype(jnp.bfloat16)
            return carry

        lax.fori_loop(0, width // wide, inner, 0, unroll=True)
        if c == 0:
            fetch(2).wait()

        def outer(t, carry):
            at = pl.ds(pl.multiple_of(t * 512, 512), 512)
            pbuf[pl.ds(before * groups, lines), at] = jnp.dot(
                hid[pl.ds(0, lines), :], down[:, at], preferred_element_type=jnp.float32
            ).astype(jnp.bfloat16)
            return carry

        lax.fori_loop(0, model_width // 512, outer, 0, unroll=True)
        to_twin(c).start()

    def pair(c):
        rows, before = chunks[c][2:]
        to_twin(c).wait_recv()
        mine = pbuf[span(before * groups, core, rows * chips), :].astype(jnp.float32)
        other = twin[pl.ds(before * chips, rows * chips), :].astype(jnp.float32)
        rsum[pl.ds(before * chips, rows * chips), :] = (mine + other).astype(jnp.bfloat16)
        for r in range(chips - 1, 0, -1):
            giving(c, r).start()
        retbuf[span(before * chips, chip, rows), :] = rsum[span(before * chips, chip, rows), :]

    def combine(c):
        start, size, rows, before = chunks[c]

        if c >= 1:
            @pl.when(layer > 0)
            def _():
                handed(c, 0).wait_recv()
                for turn in range(size):
                    xin[start + turn] = cin[0, start + turn]

        for r in range(1, chips):
            given(c, r).wait_recv()
        parts = []
        for j in range(LOCAL):
            total = None
            for i in range(per_expert):
                low = before * chips + (j * per_expert + i) * rows
                piece = retbuf[pl.ds(low, rows), :].astype(jnp.float32)
                total = piece if total is None else total + piece
            parts.append(total)
        made = jnp.concatenate(parts, axis=0).astype(jnp.bfloat16)
        tokens = size * tok_rows
        lane = lax.broadcasted_iota(jnp.int32, (tokens, LOCAL * rows), 1).astype(jnp.float32)
        at = pl.ds(start * tok_rows, tokens)
        spread = jnp.zeros((tokens, LOCAL * rows), jnp.float32)
        for k in range(2):
            spread = spread + jnp.where(lane == cols[2 * k, at, :], cols[2 * k + 1, at, :], 0.0)
        coarse = spread.astype(jnp.bfloat16).astype(jnp.float32)
        both = jnp.concatenate([coarse, spread - coarse], axis=0).astype(jnp.bfloat16)
        share = jnp.dot(both, made, preferred_element_type=jnp.float32)
        share = share[:tokens] + share[tokens:]
        for turn in range(size):
            piece = share[turn * tok_rows : (turn + 1) * tok_rows]
            summed = xin[start + turn].astype(jnp.float32) + piece
            fbuf[start + turn] = jnp.where(half == 0, summed, piece).astype(jnp.bfloat16)

        if c == 0:
            @pl.when(inner_layer)
            def _():
                hand_on(c, 1).start()
                hand_on(c, 0).start()

        @pl.when(leads(c) | ((half == 0) & (layer == layers - 1)))
        def _():
            to_partner(c).start()

        @pl.when(half == 0)
        def _():
            for turn in range(size):
                out[start + turn] = fbuf[start + turn]

    def total(c):
        start, size = chunks[c][:2]
        to_partner(c).wait_recv()
        for turn in range(size):
            at = start + turn
            whole[at] = (hin[at].astype(jnp.float32) + fbuf[at].astype(jnp.float32)).astype(jnp.bfloat16)

    def lead(c):
        @pl.when(leads(c))
        def _():
            total(c)
            dispatch_over(c, 1, whole, next_layer)
            hand_whole(c).start()

    def finish(c):
        start, size = chunks[c][:2]

        @pl.when((half == 1) & ~leads(c))
        def _():
            total(c)

        @pl.when(half == 1)
        def _():
            for turn in range(size):
                out[start + turn] = whole[start + turn]

    def first(c):
        @pl.when((layer == 0) & (core == 0))
        def _():
            dispatch(c)

    def later(c):
        start, size = chunks[c][:2]

        @pl.when(layer > 0)
        def _():
            handed(c, 0).wait_recv()
            handed(c, 1).wait_recv()
            for turn in range(size):
                at = start + turn
                xin[at] = (cin[0, at].astype(jnp.float32) + cin[1, at].astype(jnp.float32)).astype(jnp.bfloat16)
            dispatch(c)

    for i in range(5):
        small(i).start()

    @pl.when(layer < 2)
    def _():
        load_tokens().start()

    greet()
    for i in range(5):
        small(i).wait()

    @pl.when(layer < 2)
    def _():
        load_tokens().wait()

    for i in range(3):
        fetch(i).start()

    first(0)
    columns()

    for c in range(count):
        @pl.when(helps(c))
        def _():
            dispatch_over(c, 0, xin, 0)
            for r in range(chips):
                direct(c, 0, r, 0).wait_send()

    later(0)
    forward(0)
    early, late = DUE
    done = []
    for c in range(count):
        compute(c)
        for other in early.get(c, ()):
            combine(other)
        pair(c)
        for other in late.get(c, ()):
            combine(other)
        for other in early.get(c, ()) + late.get(c, ()):
            lead(other)
            done.append(other)
        if c + 1 < count:
            forward(c + 1)
    for c in range(count):
        if c not in done:
            combine(c)
            lead(c)

    @pl.when((half == 0) & inner_layer)
    def _():
        to_partner(0).start()

    for c in range(count):
        finish(c)

    for c in range(count):
        to_twin(c).wait_send()
        for r in range(1, chips):
            relay(c, r).wait_send()
            giving(c, r).wait_send()

    for c in range(count):
        @pl.when(places_own(c))
        def _():
            own_rows(c).wait_send()
            for r in range(1, chips):
                direct(c, 0, r, layer).wait_send()

        @pl.when(~places_own(c))
        def _():
            relay(c, 0).wait_send()

        @pl.when(leads(c))
        def _():
            hand_whole(c).wait_send()
            for r in range(chips):
                direct(c, 1, r, next_layer).wait_send()

        @pl.when((half == 0) | leads(c))
        def _():
            to_partner(c).wait_send()

    @pl.when(inner_layer)
    def _():
        hand_on(0, 0).wait_send()
        hand_on(0, 1).wait_send()


def on_device(tokens, norm_gain, w_gate, w_up, w_down, expert_ids, slot_ids, dropped, gate_weights):
    groups = lax.axis_size("expert")
    layers = lax.axis_size("section") // 2
    micro_count, tok_rows, model_width = tokens.shape
    width = w_gate.shape[-1]
    capacity = 5 * tok_rows // (4 * LOCAL)
    chunks, total = plan(micro_count, capacity)
    chips = groups // CORES
    count = len(chunks)
    most = max(rows for _, _, rows, _ in chunks)

    def by_choice(value):
        return jnp.transpose(value, (0, 1, 3, 2))

    vm = pl.BlockSpec(memory_space=pltpu.VMEM)
    hb = pl.BlockSpec(memory_space=pl.ANY)
    half16 = jnp.bfloat16
    dma = pltpu.SemaphoreType.DMA
    choices = (layers, micro_count, 2, tok_rows)
    state = (micro_count, tok_rows, model_width)
    made = pl.pallas_call(
        functools.partial(kernel, groups, layers, chunks, capacity),
        out_shape=jax.ShapeDtypeStruct(state, half16),
        in_specs=[hb] * 9,
        out_specs=vm,
        scratch_shapes=[
            pltpu.VMEM(norm_gain.shape, jnp.float32),
            pltpu.VMEM(choices, jnp.int32),
            pltpu.VMEM(choices, jnp.int32),
            pltpu.VMEM(choices, jnp.int32),
            pltpu.VMEM(choices, jnp.float32),
            pltpu.VMEM((model_width, width), half16),
            pltpu.VMEM((model_width, width), half16),
            pltpu.VMEM((width, model_width), half16),
            pltpu.VMEM((total * groups, model_width), half16),
            pltpu.VMEM((2, total * LOCAL, model_width), half16),
            pltpu.VMEM((total * groups, model_width), half16),
            pltpu.VMEM((total * chips, model_width), half16),
            pltpu.VMEM((total * chips, model_width), half16),
            pltpu.VMEM((total * chips, model_width), half16),
            pltpu.VMEM(state, half16),
            pltpu.VMEM(state, half16),
            pltpu.VMEM((2,) + state, half16),
            pltpu.VMEM(state, half16),
            pltpu.VMEM(state, half16),
            pltpu.VMEM((groups * most, width), half16),
            pltpu.VMEM((2, 2 * micro_count, tok_rows), jnp.float32),
            pltpu.VMEM((4, micro_count * tok_rows, 1), jnp.float32),
            dma((3,)),
            dma,
            dma((5,)),
            dma((2, count, chips)),
            dma((count, groups)),
            dma((count, chips)),
            dma((count,)),
            dma((count,)),
            dma((count, chips)),
            dma((count, chips)),
            dma((2, count)),
            dma((2, count)),
            dma((count,)),
            dma((count,)),
        ],
        compiler_params=pltpu.CompilerParams(
            collective_id=0, has_side_effects=True, vmem_limit_bytes=58 * 1024 * 1024
        ),
    )(
        tokens, norm_gain, by_choice(expert_ids), by_choice(slot_ids), by_choice(dropped), by_choice(gate_weights),
        w_gate, w_up, w_down,
    )
    return made[None]


def solution(mesh):
    return jax.shard_map(
        on_device,
        mesh=mesh,
        in_specs=(
            P(None, "expert", None),
            P(),
            P("section", None, "expert"),
            P("section", None, "expert"),
            P("section", "expert", None),
            P(None, None, "expert", None),
            P(None, None, "expert", None),
            P(None, None, "expert", None),
            P(None, None, "expert", None),
        ),
        out_specs=P("section", None, "expert", None),
        check_vma=False,
    )
```
